32 devices in a mesh: rep: 1, dp: 32 (over x, y, z, core).
Axes of the slice: x: 2, y: 2, z: 4, core: 2. Of those that a mesh axis runs over, the one named last changes fastest.
Arguments:
- x: bfloat16 [32, 2048, 1024], P(('rep', 'dp'))
- dy: bfloat16 [32, 2048, 1024], P(('rep', 'dp'))
- w_gate: bfloat16 [2, 1024, 3200], replicated
- w_up: bfloat16 [2, 1024, 3200], replicated
- w_down: bfloat16 [2, 3200, 1024], replicated
- m_w_gate: float32 [2, 1024, 3200], P(None, 'dp')
- m_w_up: float32 [2, 1024, 3200], P(None, 'dp')
- m_w_down: float32 [2, 3200, 1024], P(None, 'dp')
- v_w_gate: float32 [2, 1024, 3200], P(None, 'dp')
- v_w_up: float32 [2, 1024, 3200], P(None, 'dp')
- v_w_down: float32 [2, 3200, 1024], P(None, 'dp')
Outputs:
- output 1: bfloat16 [2, 1024, 3200], P('rep')
- output 2: bfloat16 [2, 1024, 3200], P('rep')
- output 3: bfloat16 [2, 3200, 1024], P('rep')
- output 4: float32 [2, 1024, 3200], P('rep', 'dp')
- output 5: float32 [2, 1024, 3200], P('rep', 'dp')
- output 6: float32 [2, 3200, 1024], P('rep', 'dp')
- output 7: float32 [2, 1024, 3200], P('rep', 'dp')
- output 8: float32 [2, 1024, 3200], P('rep', 'dp')
- output 9: float32 [2, 3200, 1024], P('rep', 'dp')
All inputs are finite; a program needn't handle non-finite values.
Results may differ from the reference program's by a relative error of at most 0.022.
Values are sent between devices in bfloat16 or wider.
A program may use at most 2 GiB of HBM per device.

```python
import jax
import jax.numpy as jnp
from jax import lax

SEQUENCES = 32
TOKENS = 2048
D = 1024
FF = 3200
LAYERS = 2
NAMES = ("w_gate", "w_up", "w_down")
SHAPES = {"w_gate": (LAYERS, D, FF), "w_up": (LAYERS, D, FF), "w_down": (LAYERS, FF, D)}


def bump(key, n, height):
    away = (jnp.arange(n, dtype=jnp.int32) - jax.random.randint(key, (), 0, n, jnp.int32)) % n
    return jnp.where(away < n // 8, height, 1.0)


def together(key, own, strength):
    shared = jax.random.normal(key, own.shape[1:], jnp.float32)
    return (own + strength * shared) * lax.rsqrt(1 + strength * strength)


def setup_inputs(seed: int = 0, part: int = 0) -> dict:
    kx, kdy, ka, kb, kz, kf, kh, kl, *keys = jax.random.split(jax.random.key(seed), 8 + 3 * len(NAMES))
    kx, kdy, ka, kb = (jax.random.fold_in(k, part) for k in (kx, kdy, ka, kb))
    kw, km, kv = (keys[i::3] for i in range(3))
    shape = (SEQUENCES, TOKENS, D)
    much_x, much_dy = jax.random.uniform(kz, (2,), jnp.float32, 0.0, 1.0)
    loud = 2.0 ** jax.random.uniform(jax.random.fold_in(kz, 1), (), jnp.float32, -1.0, 2.0)
    layers = 2.0 ** jax.random.uniform(kl, (LAYERS, 1, 1), jnp.float32, -1.0, 1.0)
    x = together(ka, jax.random.normal(kx, shape, jnp.float32), much_x) * bump(kf, D, 4.0)
    dy = together(kb, jax.random.normal(kdy, shape, jnp.float32), much_dy)
    drawn = {"x": x.astype(jnp.bfloat16), "dy": (loud * dy * (SEQUENCES * TOKENS) ** -0.5).astype(jnp.bfloat16)}
    for key, name in zip(kw, NAMES, strict=True):
        w = jax.random.normal(key, SHAPES[name], jnp.float32) * SHAPES[name][1] ** -0.5
        drawn[name] = (w * {"w_gate": 1.0, "w_up": bump(kh, FF, 4.0), "w_down": layers}[name]).astype(jnp.bfloat16)
    for key, name in zip(km, NAMES, strict=True):
        drawn[f"m_{name}"] = 0.1 * jax.random.normal(key, SHAPES[name], jnp.float32)
    for key, name in zip(kv, NAMES, strict=True):
        drawn[f"v_{name}"] = jax.random.uniform(key, SHAPES[name], jnp.float32, 0.005, 0.015)
    return drawn


def matmul(a, w):
    return jnp.dot(a, w, preferred_element_type=jnp.float32).astype(jnp.bfloat16)


def normed(h):
    wide = h.astype(jnp.float32)
    scale = lax.rsqrt(jnp.mean(wide**2, -1, keepdims=True) + 1e-6)
    return (wide * scale).astype(jnp.bfloat16)


def layer(h, w):
    a = normed(h)
    gate = jnp.dot(a, w["w_gate"], preferred_element_type=jnp.float32)
    up = jnp.dot(a, w["w_up"], preferred_element_type=jnp.float32)
    return h + matmul((jax.nn.silu(gate) * up).astype(jnp.bfloat16), w["w_down"])


def adamw(w, m, v, g):
    m = 0.9 * m + 0.1 * g
    v = 0.95 * v + 0.05 * g * g
    step = m * lax.rsqrt(v + 1e-8) + 0.1 * w
    return (w - 0.02 * step).astype(jnp.bfloat16), m, v


def clipped(gradients, sum_of_squares, count):
    factor = jnp.minimum(1.0, 0.5 * lax.rsqrt(sum_of_squares / count + 1e-30))
    return [g * factor for g in gradients]


def stack(weights, h):
    return lax.scan(lambda h, w: (layer(h, w), None), h, weights)[0]


def reference(x, dy, w_gate, w_up, w_down, m_w_gate, m_w_up, m_w_down, v_w_gate, v_w_up, v_w_down):
    weights = dict(zip(NAMES, (w_gate, w_up, w_down), strict=True))

    def take(so_far, sequence):
        h, by_y = sequence
        _, back = jax.vjp(lambda w: stack(w, h), weights)
        return jax.tree.map(lambda total, term: total + term.astype(jnp.float32), so_far, back(by_y)[0]), None

    none_yet = {name: jnp.zeros(w.shape, jnp.float32) for name, w in weights.items()}
    by_weights, _ = lax.scan(take, none_yet, (x, dy))
    gradients = [by_weights[name].astype(jnp.bfloat16).astype(jnp.float32) for name in NAMES]
    gradients = clipped(gradients, sum(jnp.sum(g * g) for g in gradients), sum(g.size for g in gradients))
    new = [
        adamw(w.astype(jnp.float32), m, v, g)
        for w, m, v, g in zip((w_gate, w_up, w_down), (m_w_gate, m_w_up, m_w_down), (v_w_gate, v_w_up, v_w_down), gradients, strict=True)
    ]
    return tuple(one[which] for which in range(3) for one in new)
```

```python
import jax
import jax.numpy as jnp
from jax import lax
from jax.sharding import PartitionSpec as P


AX = "dp"
f32, bf16 = jnp.float32, jnp.bfloat16


def matmul(a, w):
    return jnp.dot(a, w, preferred_element_type=f32).astype(bf16)


def normed(h):
    wide = h.astype(f32)
    scale = lax.rsqrt(jnp.mean(wide**2, -1, keepdims=True) + 1e-6)
    return (wide * scale).astype(bf16)


def layer(h, w_gate, w_up, w_down):
    a = normed(h)
    gate = jnp.dot(a, w_gate, preferred_element_type=f32)
    up = jnp.dot(a, w_up, preferred_element_type=f32)
    return h + matmul((jax.nn.silu(gate) * up).astype(bf16), w_down)


def adamw(w, m, v, g):
    m = 0.9 * m + 0.1 * g
    v = 0.95 * v + 0.05 * g * g
    step = m * lax.rsqrt(v + 1e-8) + 0.1 * w
    return (w - 0.02 * step).astype(bf16), m, v


def dev(x, y, z, c):
    return x * 16 + y * 8 + z * 2 + c


ALL = [(x, y, z, c) for x in range(2) for y in range(2) for z in range(4) for c in range(2)]
CORE = [(dev(x, y, z, c), dev(x, y, z, 1 - c)) for x, y, z, c in ALL]
FIRST = [(dev(x, y, z, c), dev(1 - x, y, z, c) if c == 0 else dev(x, 1 - y, z, c)) for x, y, z, c in ALL]
SECOND = [(dev(x, y, z, c), dev(x, 1 - y, z, c) if c == 0 else dev(1 - x, y, z, c)) for x, y, z, c in ALL]


def rising(s):
    return [(dev(x, y, z, c), dev(x, y, z + 1, c)) for x, y, z, c in ALL if z <= s - 1 and z < 3]


def falling(s):
    return [(dev(x, y, z, c), dev(x, y, z - 1, c)) for x, y, z, c in ALL if z >= 4 - s and z > 0]


def coords():
    d = lax.axis_index(AX)
    return d // 16, (d // 8) % 2, (d // 2) % 4, d % 2


def send(t, pairs):
    return lax.ppermute(t.astype(bf16), AX, pairs)


def pick(t, i, axis=0):
    return lax.dynamic_index_in_dim(t, i, axis, keepdims=False)


def over_chips(mine, theirs):
    x, y, z, c = coords()
    near = jnp.where(c == 0, (1 - x) * 2 + y, x * 2 + (1 - y))
    far = (1 - x) * 2 + (1 - y)
    onward = jnp.where(c == 0, x * 2 + (1 - y), (1 - x) * 2 + y)
    home = x * 2 + y

    def total(i):
        return pick(mine, i).astype(f32) + pick(theirs, i).astype(f32)

    got_far = send(total(far), FIRST)
    got_near = send(total(near), FIRST)
    got_second = send(total(onward) + got_far.astype(f32), SECOND)
    kept = total(home) + got_near.astype(f32) + got_second.astype(f32)
    up = down = None
    for s in (1, 2, 3):
        u = pick(kept, jnp.clip(4 - s + z, 0, 3))
        d = pick(kept, jnp.clip(z + s - 4, 0, 3))
        if up is not None:
            u, d = u + up.astype(f32), d + down.astype(f32)
        up, down = send(u, rising(s)), send(d, falling(s))
    return pick(kept, z) + up.astype(f32) + down.astype(f32)


def sum_rows(t):
    c = coords()[3]
    t = t.reshape(4, 4, 2, 32, t.shape[-1])
    theirs = send(pick(t, 1 - c, 2), CORE)
    return over_chips(pick(t, c, 2), theirs).astype(bf16)


def sum_down(t):
    c = coords()[3]
    half = t.shape[-1] // 2
    t = t.reshape(4, 4, 200, t.shape[-1])
    theirs = send(lax.dynamic_slice_in_dim(t, (1 - c) * half, half, 3), CORE)
    done = over_chips(lax.dynamic_slice_in_dim(t, c * half, half, 3), theirs).astype(bf16).reshape(2, 100, half)
    own, got = pick(done, c), send(pick(done, 1 - c), CORE)
    return jnp.where(c == 0, jnp.concatenate([own, got], 1), jnp.concatenate([got, own], 1))


def solution(mesh):
    def step(x, dy, *arrays):
        weights, moments, squares = arrays[0:3], arrays[3:6], arrays[6:9]
        layers = weights[0].shape[0]
        flat = [w[n] for n in range(layers) for w in weights]

        def stack(*flat):
            h = x[0]
            for n in range(layers):
                h = layer(h, *flat[3 * n : 3 * n + 3])
            return h

        _, back = jax.vjp(stack, *flat)
        by_weights = back(dy[0])
        sums = [None] * len(flat)
        for n in reversed(range(layers)):
            for k in (2, 1, 0):
                sums[3 * n + k] = (sum_down if k == 2 else sum_rows)(by_weights[3 * n + k])
        gradients = [jnp.stack([sums[3 * n + k] for n in range(layers)]).astype(f32) for k in range(3)]
        count = sum(w.size for w in weights)
        squared = lax.psum(sum(jnp.sum(g * g) for g in gradients), AX)
        factor = jnp.minimum(1.0, 0.5 * lax.rsqrt(squared / count + 1e-30))
        d = lax.axis_index(AX)
        new = []
        for w, m, v, g in zip(weights, moments, squares, gradients, strict=True):
            rows = m.shape[1]
            own = lax.dynamic_slice_in_dim(w, d * rows, rows, 1).astype(f32)
            new.append(adamw(own, m, v, g * factor))
        whole = [lax.all_gather(n[0], AX, axis=1, tiled=True) for n in new]
        return (*whole, *(n[1] for n in new), *(n[2] for n in new))

    whole, rows = P(None, None, None), P(None, AX, None)
    token = P(("rep", AX), None, None)
    return jax.shard_map(
        step,
        mesh=mesh,
        in_specs=(token, token, *[whole] * 3, *[rows] * 6),
        out_specs=(*[P("rep", None, None)] * 3, *[P("rep", AX, None)] * 6),
        check_vma=False,
    )
```

```python
import jax
import jax.numpy as jnp
from jax import lax
from jax.experimental import pallas as pl
from jax.experimental.pallas import tpu as pltpu
from jax.sharding import PartitionSpec as P


AX = "dp"
f32, bf16 = jnp.float32, jnp.bfloat16


def matmul(a, w):
    return jnp.dot(a, w, preferred_element_type=f32).astype(bf16)


def normed(h):
    wide = h.astype(f32)
    scale = lax.rsqrt(jnp.mean(wide**2, -1, keepdims=True) + 1e-6)
    return (wide * scale).astype(bf16)


def layer(h, w_gate, w_up, w_down):
    a = normed(h)
    gate = jnp.dot(a, w_gate, preferred_element_type=f32)
    up = jnp.dot(a, w_up, preferred_element_type=f32)
    return h + matmul((jax.nn.silu(gate) * up).astype(bf16), w_down)


def adamw(w, m, v, g):
    m = 0.9 * m + 0.1 * g
    v = 0.95 * v + 0.05 * g * g
    step = m * lax.rsqrt(v + 1e-8) + 0.1 * w
    return (w - 0.02 * step).astype(bf16), m, v


def dev(x, y, z, c):
    return x * 16 + y * 8 + z * 2 + c


ALL = [(x, y, z, c) for x in range(2) for y in range(2) for z in range(4) for c in range(2)]
CORE = [(dev(x, y, z, c), dev(x, y, z, 1 - c)) for x, y, z, c in ALL]
FIRST = [(dev(x, y, z, c), dev(1 - x, y, z, c) if c == 0 else dev(x, 1 - y, z, c)) for x, y, z, c in ALL]
SECOND = [(dev(x, y, z, c), dev(x, 1 - y, z, c) if c == 0 else dev(1 - x, y, z, c)) for x, y, z, c in ALL]


NEXT = [(dev(x, y, z, c), dev(x, y, z ^ 1, c)) for x, y, z, c in ALL]
AFTER = [(dev(x, y, z, c), dev(x, y, z ^ 2, c)) for x, y, z, c in ALL]


def coords():
    d = lax.axis_index(AX)
    return d // 16, (d // 8) % 2, (d // 2) % 4, d % 2


def send(t, pairs):
    return lax.ppermute(t.astype(bf16), AX, pairs)


def pick(t, i, axis=0):
    return lax.dynamic_index_in_dim(t, i, axis, keepdims=False)


class Sum:
    def __init__(self, mine, other):
        self.mine, self.other = mine, other

    def total(self, i):
        return pick(self.mine, i).astype(f32) + pick(self.theirs, i).astype(f32)

    def over_cores(self):
        self.theirs = send(self.other, CORE)

    def over_first(self):
        x, y, z, c = coords()
        self.got_far = send(self.total((1 - x) * 2 + (1 - y)), FIRST)
        self.got_near = send(self.total(jnp.where(c == 0, (1 - x) * 2 + y, x * 2 + (1 - y))), FIRST)

    def over_second(self):
        x, y, z, c = coords()
        onward = jnp.where(c == 0, x * 2 + (1 - y), (1 - x) * 2 + y)
        self.got_second = send(self.total(onward) + self.got_far.astype(f32), SECOND)

    def over_line(self):
        x, y, z, c = coords()
        kept = self.total(x * 2 + y) + self.got_near.astype(f32) + self.got_second.astype(f32)
        beside = z + 1 - 2 * (z % 2)
        got = send(jnp.stack([pick(kept, beside), pick(kept, 3 - z)]), NEXT)
        last = send(pick(kept, (z + 2) % 4) + got[1].astype(f32), AFTER)
        return (pick(kept, z) + got[0].astype(f32) + last.astype(f32)).astype(bf16)


def sum_of_rows(*ts):
    c = coords()[3]
    ts = [t.reshape(4, 4, 2, 32, t.shape[-1]) for t in ts]
    part = lambda i: jnp.concatenate([pick(t, i, 2) for t in ts], 2)
    return Sum(part(c), part(1 - c))


def sum_of_down(t):
    c = coords()[3]
    half = t.shape[-1] // 2
    t = t.reshape(4, 4, 200, t.shape[-1])
    part = lambda i: lax.dynamic_slice_in_dim(t, i * half, half, 3)
    return Sum(part(c), part(1 - c))


def in_core_order(own, got, axis):
    c = coords()[3]
    return jnp.where(c == 0, jnp.concatenate([own, got], axis), jnp.concatenate([got, own], axis))


def down_rows(done):
    c = coords()[3]
    done = done.reshape(2, 100, done.shape[-1])
    return in_core_order(pick(done, c), send(pick(done, 1 - c), CORE), 1)


def remote(src, dst, send_sem, recv_sem, to):
    return pltpu.make_async_remote_copy(
        src_ref=src, dst_ref=dst, send_sem=send_sem, recv_sem=recv_sem, device_id={AX: to}, device_id_type=pl.DeviceIdType.MESH
    )


def meet(partners):
    barrier = pltpu.get_barrier_semaphore()
    for p in partners:
        pl.semaphore_signal(barrier, inc=1, device_id={AX: p}, device_id_type=pl.DeviceIdType.MESH)
    pl.semaphore_wait(barrier, len(partners))


def gather_kernel(gate_in, up_in, down_in, gate, up, down, send_sem, near_sem, from_z, from_second, from_first, from_core):
    x, y, z, c = coords()
    me = dev(x, y, z, c)
    flip_x, flip_y = 1 - 2 * x, 1 - 2 * y
    first = (x + (1 - c) * flip_x, y + c * flip_y)
    second = (x + c * flip_x, y + (1 - c) * flip_y)
    both = (1 - x, 1 - y)
    beside, farthest = 1 + z % 2, 3 * (1 - z // 2)
    line = [z, beside, 6 - z - beside - farthest, farthest]
    to_first, to_second, to_core = dev(*first, z, c), dev(*second, z, c), dev(x, y, z, 1 - c)
    meet([dev(x, y, zz, c) for zz in line[1:]] + [to_first, to_second, to_core])

    def block(owner):
        chip = pl.ds(pl.multiple_of(owner // 2 * 200, 8), 200)
        rows = pl.ds(pl.multiple_of(owner * 32, 32), 32)
        return gate.at[:, rows, :], up.at[:, rows, :], down.at[owner % 2, chip, :]

    sent = []

    def push(owner, to, sem, i, src=None):
        for j, (s, d) in enumerate(zip(src or block(owner), block(owner), strict=True)):
            copy = remote(s, d, send_sem.at[len(sent)], sem.at[i, j], to)
            copy.start()
            sent.append(copy)

    def arrived(owner, sem, i):
        for j, d in enumerate(block(owner)):
            remote(d, d, send_sem.at[0], sem.at[i, j], to_core).wait_recv()

    own = (gate_in, up_in, down_in)
    for zz in line[1:]:
        push(me, dev(x, y, zz, c), from_z, z, own)
        if zz is line[1]:
            push(me, to_second, from_second, z, own)
            push(me, to_first, from_first, z, own)
    push(me, to_core, from_core, z, own)
    near = [pltpu.make_async_copy(s, d, near_sem.at[j]) for j, (s, d) in enumerate(zip(own, block(me), strict=True))]
    for copy in near:
        copy.start()
    def of_line(zz):
        owner = dev(x, y, zz, c)
        arrived(owner, from_z, zz)
        push(owner, to_second, from_second, zz)
        push(owner, to_first, from_first, zz)
        push(owner, to_core, from_core, zz)

    def of_second(zz):
        owner = dev(*second, zz, c)
        arrived(owner, from_second, zz)
        push(owner, to_first, from_first, 4 + zz)
        push(owner, to_core, from_core, 4 + zz)

    for k in (1, 2, 3):
        of_line(line[k])
        of_second(line[k - 1])
    of_second(line[3])
    for w, place in enumerate((first, both)):
        for zz in line:
            owner = dev(*place, zz, c)
            arrived(owner, from_first, 4 * w + zz)
            push(owner, to_core, from_core, 8 + 4 * w + zz)
    for w, place in enumerate(((x, y), first, second, both)):
        for zz in line:
            arrived(dev(*place, zz, 1 - c), from_core, 4 * w + zz)
    for copy in near:
        copy.wait()
    for copy in sent:
        copy.wait_send()


def gathered(gate, up, down):
    devices = len(ALL)
    shapes = [(t.shape[0], t.shape[1] * devices, t.shape[2]) for t in (gate, up)]
    shapes.append((2, down.shape[0] * devices // 2, down.shape[1]))
    return pl.pallas_call(
        gather_kernel,
        out_shape=[jax.ShapeDtypeStruct(shape, bf16) for shape in shapes],
        in_specs=[pl.BlockSpec(memory_space=pl.ANY)] * 3,
        out_specs=[pl.BlockSpec(memory_space=pl.ANY)] * 3,
        scratch_shapes=[
            pltpu.SemaphoreType.DMA((93,)),
            pltpu.SemaphoreType.DMA((3,)),
            pltpu.SemaphoreType.DMA((4, 3)),
            pltpu.SemaphoreType.DMA((4, 3)),
            pltpu.SemaphoreType.DMA((8, 3)),
            pltpu.SemaphoreType.DMA((16, 3)),
        ],
        compiler_params=pltpu.CompilerParams(collective_id=0, has_side_effects=True),
    )(gate, up, down)


def product_kernel(a, w_gate, w_up, gate, up, p):
    g = jnp.dot(a[...], w_gate[...], preferred_element_type=f32)
    u = jnp.dot(a[...], w_up[...], preferred_element_type=f32)
    gate[...] = g
    up[...] = u
    p[...] = (jax.nn.silu(g) * u).astype(bf16)


def product(a, w_gate, w_up):
    tokens, d = a.shape
    ff = w_gate.shape[2]
    rows, columns = 512, 640
    weight = pl.BlockSpec((None, d, columns), lambda j, i: (0, 0, j))
    tile = pl.BlockSpec((rows, columns), lambda j, i: (i, j))
    return pl.pallas_call(
        product_kernel,
        grid=(ff // columns, tokens // rows),
        in_specs=[pl.BlockSpec((rows, d), lambda j, i: (i, 0)), weight, weight],
        out_specs=[tile] * 3,
        out_shape=[jax.ShapeDtypeStruct((tokens, ff), t) for t in (f32, f32, bf16)],
        compiler_params=pltpu.CompilerParams(vmem_limit_bytes=48 * 1024 * 1024),
        cost_estimate=pl.CostEstimate(flops=4 * tokens * d * ff, bytes_accessed=10 * tokens * ff + 4 * d * ff, transcendentals=tokens * ff),
    )(a, w_gate, w_up)


def add_up_kernel(term, total, heard, send_sem, recv_sem):
    me = lax.axis_index(AX)
    others = [(me + k) % len(ALL) for k in range(1, len(ALL))]
    meet(others)
    copies = [remote(term, heard.at[me], send_sem.at[k], recv_sem.at[me], to) for k, to in enumerate(others)]
    for copy in copies:
        copy.start()
    for to in others:
        remote(term, heard.at[to], send_sem.at[0], recv_sem.at[to], to).wait_recv()
    so_far = term[...]
    for to in others:
        so_far += heard[to]
    total[...] = so_far
    for copy in copies:
        copy.wait_send()


def added_up(term):
    n = len(ALL)
    return pl.pallas_call(
        add_up_kernel,
        out_shape=jax.ShapeDtypeStruct((8, 128), f32),
        in_specs=[pl.BlockSpec(memory_space=pltpu.VMEM)],
        out_specs=pl.BlockSpec(memory_space=pltpu.VMEM),
        scratch_shapes=[pltpu.VMEM((n, 8, 128), f32), pltpu.SemaphoreType.DMA((n - 1,)), pltpu.SemaphoreType.DMA((n,))],
        compiler_params=pltpu.CompilerParams(collective_id=1, has_side_effects=True),
    )(jnp.full((8, 128), term, f32))[0, 0]


def solution(mesh):
    def step(x, dy, *arrays):
        weights, moments, squares = arrays[0:3], arrays[3:6], arrays[6:9]
        down_0, later = weights[2][0], [w[1] for w in weights]
        h, dh = x[0], dy[0]
        a = normed(h)
        gate, up, p = product(a, *weights[:2])
        _, back_p = jax.vjp(lambda gate, up: (jax.nn.silu(gate) * up).astype(bf16), gate, up)
        _, back = jax.vjp(layer, h + matmul(p, down_0), *later)
        dh, *by_later = back(dh)
        dh, *by_later = lax.optimization_barrier((dh, *by_later))
        rows_1, down_1 = sum_of_rows(*by_later[:2]), sum_of_down(by_later[2])
        down_1.over_cores()
        rows_1.over_cores()
        dp = lax.dot_general(dh, down_0, (((1,), (1,)), ((), ())), preferred_element_type=f32).astype(bf16)
        d_gate, d_up = (t.astype(bf16) for t in back_p(dp))
        d_gate, d_up, p, down_1.theirs, rows_1.theirs = lax.optimization_barrier((d_gate, d_up, p, down_1.theirs, rows_1.theirs))
        down_1.over_first()
        rows_1.over_first()

        def by(left, right):
            return lax.dot_general(left, right, (((0,), (0,)), ((), ())), preferred_element_type=f32).astype(bf16)

        by_down, by_gate = by(p, dh), by(a, d_gate)
        down_0 = sum_of_down(by_down)
        down_0.over_cores()
        d_up, by_gate, down_1.got_far, rows_1.got_far, down_0.theirs = lax.optimization_barrier(
            (d_up, by_gate, down_1.got_far, rows_1.got_far, down_0.theirs)
        )
        down_1.over_second()
        rows_1.over_second()
        rows_0 = sum_of_rows(by_gate, by(a, d_up))
        rows_0.over_cores()
        down_0.over_first()
        rows_0.over_first()
        down_0.over_second()
        rows_0.over_second()
        both_rows = [s.over_line() for s in (rows_0, rows_1)]
        gradients = [jnp.stack([r[32 * k : 32 * (k + 1)] for r in both_rows]).astype(f32) for k in range(2)]
        gradients.append(jnp.stack([down_rows(s.over_line()) for s in (down_0, down_1)]).astype(f32))
        count = sum(w.size for w in weights)
        squared = added_up(sum(jnp.sum(g * g) for g in gradients))
        factor = jnp.minimum(1.0, 0.5 * lax.rsqrt(squared / count + 1e-30))
        d = lax.axis_index(AX)
        new = []
        for w, m, v, g in zip(weights, moments, squares, gradients, strict=True):
            rows = m.shape[1]
            own = lax.dynamic_slice_in_dim(w, d * rows, rows, 1).astype(f32)
            new.append(adamw(own, m, v, g * factor))
        c = coords()[3]
        chip = in_core_order(pick(new[2][0], c), send(pick(new[2][0], 1 - c), CORE), 0)
        whole = gathered(new[0][0], new[1][0], chip)
        return (*whole, *(n[1] for n in new), *(n[2] for n in new))

    whole, rows = P(None, None, None), P(None, AX, None)
    token = P(("rep", AX), None, None)
    return jax.shard_map(
        step,
        mesh=mesh,
        in_specs=(token, token, *[whole] * 3, *[rows] * 6),
        out_specs=(*[P("rep", None, None)] * 3, *[P("rep", AX, None)] * 6),
        check_vma=False,
    )
```

```python
import jax
import jax.numpy as jnp
from jax import lax
from jax.experimental import pallas as pl
from jax.experimental.pallas import tpu as pltpu
from jax.sharding import PartitionSpec as P


AX = "dp"
f32, bf16 = jnp.float32, jnp.bfloat16


def matmul(a, w):
    return jnp.dot(a, w, preferred_element_type=f32).astype(bf16)


def normed(h):
    wide = h.astype(f32)
    scale = lax.rsqrt(jnp.mean(wide**2, -1, keepdims=True) + 1e-6)
    return (wide * scale).astype(bf16)


def layer(h, w_gate, w_up, w_down):
    a = normed(h)
    gate = jnp.dot(a, w_gate, preferred_element_type=f32)
    up = jnp.dot(a, w_up, preferred_element_type=f32)
    return h + matmul((jax.nn.silu(gate) * up).astype(bf16), w_down)


def adamw(w, m, v, g):
    m = 0.9 * m + 0.1 * g
    v = 0.95 * v + 0.05 * g * g
    step = m * lax.rsqrt(v + 1e-8) + 0.1 * w
    return (w - 0.02 * step).astype(bf16), m, v


def dev(x, y, z, c):
    return x * 16 + y * 8 + z * 2 + c


ALL = [(x, y, z, c) for x in range(2) for y in range(2) for z in range(4) for c in range(2)]
CORE = [(dev(x, y, z, c), dev(x, y, z, 1 - c)) for x, y, z, c in ALL]
FIRST = [(dev(x, y, z, c), dev(1 - x, y, z, c) if c == 0 else dev(x, 1 - y, z, c)) for x, y, z, c in ALL]
SECOND = [(dev(x, y, z, c), dev(x, 1 - y, z, c) if c == 0 else dev(1 - x, y, z, c)) for x, y, z, c in ALL]


NEXT = [(dev(x, y, z, c), dev(x, y, z ^ 1, c)) for x, y, z, c in ALL]
AFTER = [(dev(x, y, z, c), dev(x, y, z ^ 2, c)) for x, y, z, c in ALL]


def coords():
    d = lax.axis_index(AX)
    return d // 16, (d // 8) % 2, (d // 2) % 4, d % 2


def send(t, pairs):
    return lax.ppermute(t.astype(bf16), AX, pairs)


def pick(t, i, axis=0):
    return lax.dynamic_index_in_dim(t, i, axis, keepdims=False)


class Sum:
    def __init__(self, mine, other):
        self.mine, self.other = mine, other

    def total(self, i):
        return pick(self.mine, i).astype(f32) + pick(self.theirs, i).astype(f32)

    def over_cores(self):
        self.theirs = send(self.other, CORE)

    def over_first(self):
        x, y, z, c = coords()
        self.got_far = send(self.total((1 - x) * 2 + (1 - y)), FIRST)
        self.got_near = send(self.total(jnp.where(c == 0, (1 - x) * 2 + y, x * 2 + (1 - y))), FIRST)

    def over_second(self):
        x, y, z, c = coords()
        onward = jnp.where(c == 0, x * 2 + (1 - y), (1 - x) * 2 + y)
        self.got_second = send(self.total(onward) + self.got_far.astype(f32), SECOND)

    def over_line(self):
        x, y, z, c = coords()
        kept = self.total(x * 2 + y) + self.got_near.astype(f32) + self.got_second.astype(f32)
        beside = z + 1 - 2 * (z % 2)
        got = send(jnp.stack([pick(kept, beside), pick(kept, 3 - z)]), NEXT)
        last = send(pick(kept, (z + 2) % 4) + got[1].astype(f32), AFTER)
        return (pick(kept, z) + got[0].astype(f32) + last.astype(f32)).astype(bf16)


def sum_of_rows(*ts):
    c = coords()[3]
    ts = [t.reshape(4, 4, 2, 32, t.shape[-1]) for t in ts]
    part = lambda i: jnp.concatenate([pick(t, i, 2) for t in ts], 2)
    return Sum(part(c), part(1 - c))


def sum_of_down(t):
    c = coords()[3]
    half = t.shape[-1] // 2
    t = t.reshape(4, 4, 200, t.shape[-1])
    part = lambda i: lax.dynamic_slice_in_dim(t, i * half, half, 3)
    return Sum(part(c), part(1 - c))


def in_core_order(own, got, axis):
    c = coords()[3]
    return jnp.where(c == 0, jnp.concatenate([own, got], axis), jnp.concatenate([got, own], axis))


def down_rows(done):
    c = coords()[3]
    done = done.reshape(2, 100, done.shape[-1])
    return in_core_order(pick(done, c), send(pick(done, 1 - c), CORE), 1)


def remote(src, dst, send_sem, recv_sem, to):
    return pltpu.make_async_remote_copy(
        src_ref=src, dst_ref=dst, send_sem=send_sem, recv_sem=recv_sem, device_id={AX: to}, device_id_type=pl.DeviceIdType.MESH
    )


def meet(partners):
    barrier = pltpu.get_barrier_semaphore()
    for p in partners:
        pl.semaphore_signal(barrier, inc=1, device_id={AX: p}, device_id_type=pl.DeviceIdType.MESH)
    pl.semaphore_wait(barrier, len(partners))


def gather_kernel(gate_in, up_in, down_in, gate, up, down, send_sem, near_sem, from_z, from_second, from_first, from_core):
    x, y, z, c = coords()
    me = dev(x, y, z, c)
    flip_x, flip_y = 1 - 2 * x, 1 - 2 * y
    first = (x + (1 - c) * flip_x, y + c * flip_y)
    second = (x + c * flip_x, y + (1 - c) * flip_y)
    both = (1 - x, 1 - y)
    beside, farthest = 1 + z % 2, 3 * (1 - z // 2)
    line = [z, beside, 6 - z - beside - farthest, farthest]
    to_first, to_second, to_core = dev(*first, z, c), dev(*second, z, c), dev(x, y, z, 1 - c)
    meet([dev(x, y, zz, c) for zz in line[1:]] + [to_first, to_second, to_core])

    def block(owner):
        chip = pl.ds(pl.multiple_of(owner // 2 * 200, 8), 200)
        rows = pl.ds(pl.multiple_of(owner * 32, 32), 32)
        return gate.at[:, rows, :], up.at[:, rows, :], down.at[owner % 2, chip, :]

    sent = []

    def push(owner, to, sem, i, src=None):
        for j, (s, d) in enumerate(zip(src or block(owner), block(owner), strict=True)):
            copy = remote(s, d, send_sem.at[len(sent)], sem.at[i, j], to)
            copy.start()
            sent.append(copy)

    def arrived(owner, sem, i):
        for j, d in enumerate(block(owner)):
            remote(d, d, send_sem.at[0], sem.at[i, j], to_core).wait_recv()

    own = (gate_in, up_in, down_in)
    for zz in line[1:]:
        push(me, dev(x, y, zz, c), from_z, z, own)
        if zz is line[1]:
            push(me, to_second, from_second, z, own)
            push(me, to_first, from_first, z, own)
    push(me, to_core, from_core, z, own)
    near = [pltpu.make_async_copy(s, d, near_sem.at[j]) for j, (s, d) in enumerate(zip(own, block(me), strict=True))]
    for copy in near:
        copy.start()
    def of_line(zz):
        owner = dev(x, y, zz, c)
        arrived(owner, from_z, zz)
        push(owner, to_second, from_second, zz)
        push(owner, to_first, from_first, zz)
        push(owner, to_core, from_core, zz)

    def of_second(zz):
        owner = dev(*second, zz, c)
        arrived(owner, from_second, zz)
        push(owner, to_first, from_first, 4 + zz)
        push(owner, to_core, from_core, 4 + zz)

    for k in (1, 2, 3):
        of_line(line[k])
        of_second(line[k - 1])
    of_second(line[3])
    for w, place in enumerate((first, both)):
        for zz in line:
            owner = dev(*place, zz, c)
            arrived(owner, from_first, 4 * w + zz)
            push(owner, to_core, from_core, 8 + 4 * w + zz)
    for w, place in enumerate(((x, y), first, second, both)):
        for zz in line:
            arrived(dev(*place, zz, 1 - c), from_core, 4 * w + zz)
    for copy in near:
        copy.wait()
    for copy in sent:
        copy.wait_send()


def gathered(gate, up, down):
    devices = len(ALL)
    shapes = [(t.shape[0], t.shape[1] * devices, t.shape[2]) for t in (gate, up)]
    shapes.append((2, down.shape[0] * devices // 2, down.shape[1]))
    return pl.pallas_call(
        gather_kernel,
        out_shape=[jax.ShapeDtypeStruct(shape, bf16) for shape in shapes],
        in_specs=[pl.BlockSpec(memory_space=pl.ANY)] * 3,
        out_specs=[pl.BlockSpec(memory_space=pl.ANY)] * 3,
        scratch_shapes=[
            pltpu.SemaphoreType.DMA((93,)),
            pltpu.SemaphoreType.DMA((3,)),
            pltpu.SemaphoreType.DMA((4, 3)),
            pltpu.SemaphoreType.DMA((4, 3)),
            pltpu.SemaphoreType.DMA((8, 3)),
            pltpu.SemaphoreType.DMA((16, 3)),
        ],
        compiler_params=pltpu.CompilerParams(collective_id=0, has_side_effects=True),
    )(gate, up, down)


def product_kernel(a, w_gate, w_up, gate, up, p):
    g = jnp.dot(a[...], w_gate[...], preferred_element_type=f32)
    u = jnp.dot(a[...], w_up[...], preferred_element_type=f32)
    gate[...] = g
    up[...] = u
    p[...] = (jax.nn.silu(g) * u).astype(bf16)


def product(a, w_gate, w_up):
    tokens, d = a.shape
    ff = w_gate.shape[2]
    rows, columns = 512, 640
    weight = pl.BlockSpec((None, d, columns), lambda j, i: (0, 0, j))
    tile = pl.BlockSpec((rows, columns), lambda j, i: (i, j))
    return pl.pallas_call(
        product_kernel,
        grid=(ff // columns, tokens // rows),
        in_specs=[pl.BlockSpec((rows, d), lambda j, i: (i, 0)), weight, weight],
        out_specs=[tile] * 3,
        out_shape=[jax.ShapeDtypeStruct((tokens, ff), t) for t in (f32, f32, bf16)],
        compiler_params=pltpu.CompilerParams(vmem_limit_bytes=48 * 1024 * 1024),
        cost_estimate=pl.CostEstimate(flops=4 * tokens * d * ff, bytes_accessed=10 * tokens * ff + 4 * d * ff, transcendentals=tokens * ff),
    )(a, w_gate, w_up)


def add_up_kernel(term, total, heard, send_sem, recv_sem):
    me = lax.axis_index(AX)
    others = [(me + k) % len(ALL) for k in range(1, len(ALL))]
    meet(others)
    copies = [remote(term, heard.at[me], send_sem.at[k], recv_sem.at[me], to) for k, to in enumerate(others)]
    for copy in copies:
        copy.start()
    for to in others:
        remote(term, heard.at[to], send_sem.at[0], recv_sem.at[to], to).wait_recv()
    so_far = term[...]
    for to in others:
        so_far += heard[to]
    total[...] = so_far
    for copy in copies:
        copy.wait_send()


def added_up(term):
    n = len(ALL)
    return pl.pallas_call(
        add_up_kernel,
        out_shape=jax.ShapeDtypeStruct((8, 128), f32),
        in_specs=[pl.BlockSpec(memory_space=pltpu.VMEM)],
        out_specs=pl.BlockSpec(memory_space=pltpu.VMEM),
        scratch_shapes=[pltpu.VMEM((n, 8, 128), f32), pltpu.SemaphoreType.DMA((n - 1,)), pltpu.SemaphoreType.DMA((n,))],
        compiler_params=pltpu.CompilerParams(collective_id=1, has_side_effects=True),
    )(jnp.full((8, 128), term, f32))[0, 0]


def solution(mesh):
    def step(x, dy, *arrays):
        weights, moments, squares = arrays[0:3], arrays[3:6], arrays[6:9]
        down_0, later = weights[2][0], [w[1] for w in weights]
        h, dh = x[0], dy[0]
        a = normed(h)
        gate, up, p = product(a, *weights[:2])
        _, back_p = jax.vjp(lambda gate, up: (jax.nn.silu(gate) * up).astype(bf16), gate, up)
        _, back = jax.vjp(layer, h + matmul(p, down_0), *later)
        dh, *by_later = back(dh)
        dh, *by_later = lax.optimization_barrier((dh, *by_later))
        rows_1, down_1 = sum_of_rows(*by_later[:2]), sum_of_down(by_later[2])
        down_1.over_cores()
        rows_1.over_cores()
        dp = lax.dot_general(dh, down_0, (((1,), (1,)), ((), ())), preferred_element_type=f32).astype(bf16)
        d_gate, d_up = (t.astype(bf16) for t in back_p(dp))
        d_gate, d_up, p, down_1.theirs, rows_1.theirs = lax.optimization_barrier((d_gate, d_up, p, down_1.theirs, rows_1.theirs))
        down_1.over_first()
        rows_1.over_first()

        def by(left, right):
            return lax.dot_general(left, right, (((0,), (0,)), ((), ())), preferred_element_type=f32).astype(bf16)

        by_down, by_gate = by(p, dh), by(a, d_gate)
        down_0 = sum_of_down(by_down)
        down_0.over_cores()
        d_up, by_gate, down_1.got_far, rows_1.got_far, down_0.theirs = lax.optimization_barrier(
            (d_up, by_gate, down_1.got_far, rows_1.got_far, down_0.theirs)
        )
        down_1.over_second()
        rows_1.over_second()
        gate_0 = sum_of_rows(by_gate)
        gate_0.over_cores()
        down_0.over_first()
        up_0 = sum_of_rows(by(a, d_up))
        up_0.over_cores()
        gate_0.over_first()
        up_0.over_first()
        down_0.over_second()
        gate_0.over_second()
        up_0.over_second()
        rows_1 = rows_1.over_line()
        gradients = [jnp.stack([s.over_line(), rows_1[32 * k : 32 * (k + 1)]]).astype(f32) for k, s in enumerate((gate_0, up_0))]
        gradients.append(jnp.stack([down_rows(s.over_line()) for s in (down_0, down_1)]).astype(f32))
        count = sum(w.size for w in weights)
        squared = added_up(sum(jnp.sum(g * g) for g in gradients))
        factor = jnp.minimum(1.0, 0.5 * lax.rsqrt(squared / count + 1e-30))
        d = lax.axis_index(AX)
        new = []
        for w, m, v, g in zip(weights, moments, squares, gradients, strict=True):
            rows = m.shape[1]
            own = lax.dynamic_slice_in_dim(w, d * rows, rows, 1).astype(f32)
            new.append(adamw(own, m, v, g * factor))
        c = coords()[3]
        chip = in_core_order(pick(new[2][0], c), send(pick(new[2][0], 1 - c), CORE), 0)
        whole = gathered(new[0][0], new[1][0], chip)
        return (*whole, *(n[1] for n in new), *(n[2] for n in new))

    whole, rows = P(None, None, None), P(None, AX, None)
    token = P(("rep", AX), None, None)
    return jax.shard_map(
        step,
        mesh=mesh,
        in_specs=(token, token, *[whole] * 3, *[rows] * 6),
        out_specs=(*[P("rep", None, None)] * 3, *[P("rep", AX, None)] * 6),
        check_vma=False,
    )
```
